128 devices in a mesh: prob: 1, samp: 2 (over core), feat: 64 (over z, y, x).
Axes of the slice: x: 4, y: 4, z: 4, core: 2. Of those that a mesh axis runs over, the one named last changes fastest.
Arguments:
- x_mat: bfloat16 [8192, 65536], P(('prob', 'samp'), 'feat')
- w_init: float32 [65536, 64], P(('prob', 'feat'))
- targets: float32 [8192, 64], P(('prob', 'samp'))
- step_size: float32 [65536], P(('prob', 'feat'))
Outputs:
- output 1: float32 [65536, 64], P(('prob', 'feat'))
- output 2: float32 [8192, 64], P(('prob', 'samp'))
All inputs are finite; a program needn't handle non-finite values.
Results may differ from the reference program's by a relative error of at most 0.00316278.
Values are sent between devices in bfloat16 or wider.
A program may use at most 1 GiB of HBM per device.

```python
import math
import jax
import jax.numpy as jnp
from jax import lax

SAMPLES = 8192
FEATURES = 65536
TARGETS = 64
FEAT_BLOCKS = 64
SWEEPS = 4
COMBINE_WEIGHT = 0.8
RIDGE_SCALE = 0.1


def feature_steps(x_mat, spread, start_key):
    col_sq = jnp.sum(jnp.square(x_mat.astype(jnp.float32)), axis=0) / SAMPLES
    precond = spread / col_sq
    root_pre = jnp.sqrt(precond)
    start_dir = jax.random.normal(start_key, (FEATURES,), jnp.float32)
    start_dir = start_dir / jnp.sqrt(jnp.sum(start_dir * start_dir))

    def power_step(direction, unused):
        row_vals = jnp.dot(x_mat, (root_pre * direction).astype(jnp.bfloat16), preferred_element_type=jnp.float32)
        col_vals = root_pre * jnp.dot(row_vals.astype(jnp.bfloat16), x_mat, preferred_element_type=jnp.float32) / SAMPLES
        dir_norm = jnp.sqrt(jnp.sum(col_vals * col_vals))
        return col_vals / dir_norm, dir_norm

    final_dir, dir_norms = lax.scan(power_step, start_dir, None, length=30)
    return precond / dir_norms[-1]


def setup_inputs(seed: int = 0, part: int = 0) -> dict:
    part_key = jax.random.fold_in(jax.random.key(seed), part)
    key_list = jax.random.split(part_key, 8)
    factor_rank = 8
    shared_frac = 2.0 * factor_rank / SAMPLES
    factors = jax.random.normal(key_list[0], (SAMPLES, factor_rank), jnp.float32)
    loadings = jax.random.normal(key_list[1], (FEATURES, factor_rank), jnp.float32)
    noise_part = jax.random.normal(key_list[2], (SAMPLES, FEATURES), jnp.float32)
    shared = jnp.dot(factors, loadings.T)
    x_mat = (math.sqrt(shared_frac / factor_rank) * shared + math.sqrt(1.0 - shared_frac) * noise_part).astype(jnp.bfloat16)
    spread = jnp.exp2(jax.random.uniform(key_list[3], (FEATURES,), jnp.float32, -2.0, 2.0))
    step_size = feature_steps(x_mat, spread, key_list[4])
    z_mat = jax.random.normal(key_list[5], (SAMPLES, TARGETS), jnp.float32).astype(jnp.bfloat16)
    w_raw = lax.dot_general(x_mat, z_mat, (((0,), (0,)), ((), ())), preferred_element_type=jnp.float32)
    w_fit = jnp.dot(x_mat, w_raw.astype(jnp.bfloat16), preferred_element_type=jnp.float32)
    w_init = w_raw * (0.7 / jnp.sqrt(jnp.mean(w_fit * w_fit)))
    w_true = jax.random.normal(key_list[6], (FEATURES, TARGETS), jnp.float32).astype(jnp.bfloat16)
    y_signal = jnp.dot(x_mat, w_true, preferred_element_type=jnp.float32)
    y_noise = jax.random.normal(key_list[7], (SAMPLES, TARGETS), jnp.float32)
    targets = 0.8 * y_signal / jnp.sqrt(jnp.mean(y_signal * y_signal)) + 0.6 * y_noise
    return {"x_mat": x_mat, "w_init": w_init, "targets": targets, "step_size": step_size}


def block_sum(x_mat, weights):
    feat_len = FEATURES // FEAT_BLOCKS
    weights_low = weights.astype(jnp.bfloat16)

    def one_block(total, block):
        x_block = lax.dynamic_slice_in_dim(x_mat, block * feat_len, feat_len, axis=1)
        w_block = lax.dynamic_slice_in_dim(weights_low, block * feat_len, feat_len, axis=0)
        block_prod = jnp.dot(x_block, w_block, preferred_element_type=jnp.float32)
        return total + block_prod.astype(jnp.bfloat16).astype(jnp.float32), None

    total, unused = lax.scan(one_block, jnp.zeros((SAMPLES, TARGETS), jnp.float32), jnp.arange(FEAT_BLOCKS))
    return total


def reference(x_mat, w_init, targets, step_size):
    ridge = RIDGE_SCALE * FEATURES / SAMPLES
    start_resid = targets - block_sum(x_mat, w_init)

    def sweep(state, unused):
        weights, residual = state
        gradient = lax.dot_general(x_mat, residual.astype(jnp.bfloat16), (((0,), (0,)), ((), ())), preferred_element_type=jnp.float32) / SAMPLES
        delta = step_size[:, None] * (gradient - ridge * weights)
        weights = weights + COMBINE_WEIGHT * delta
        residual = residual - COMBINE_WEIGHT * block_sum(x_mat, delta)
        return (weights, residual), None

    (weights, residual), unused = lax.scan(sweep, (w_init, start_resid), None, length=SWEEPS)
    return weights, residual
```

```python
import jax
import jax.numpy as jnp
from jax import lax
from jax.experimental import pallas as pl
from jax.experimental.pallas import tpu as pltpu
from jax.sharding import PartitionSpec as P

SWEEPS = 4
COMBINE_WEIGHT = 0.8
RIDGE_SCALE = 0.1
SIDE = 4
MESH_ID = pl.DeviceIdType.MESH

PLANE = sorted(
    [(dx, dy) for dy in range(SIDE) for dx in range(SIDE)],
    key=lambda d: -(min(d[0], SIDE - d[0]) + min(d[1], SIDE - d[1])),
)
FAR_FIRST = (2, 1, 3, 0)
NEAR_FIRST = (0, 1, 3, 2)


def solution(mesh):
    samp_count = mesh.shape["samp"]
    feat_count = mesh.shape["feat"]
    assert feat_count == SIDE**3 and samp_count == 2

    def make_kernel(rows, feat_len, targets, ridge, samples):
        half = rows // 2
        chunk = half // feat_count
        plane = half // SIDE
        lanes = 2 * targets
        f32, bf16 = jnp.float32, jnp.bfloat16

        def kernel(x_hbm, w_hbm, y_hbm, eta_ref, wt_out, rp_out, x_v, w_v, y_v, ub, rs, rb, rown, rf, wt, gacc, gx, wl, wr,
                   x_sem, in_sem, rs_send, rs_recv, ag_send, ag_recv, gx_send, gx_recv, out_sem):
            samp = lax.axis_index("samp")
            me = lax.axis_index("feat")
            cx, cy, cz = me % SIDE, (me // SIDE) % SIDE, me // (SIDE * SIDE)
            nx = [(cx + d) % SIDE for d in range(SIDE)]
            ny = [((cy + d) % SIDE) * SIDE for d in range(SIDE)]
            nz = [(cz + d) % SIDE for d in range(SIDE)]
            sibling = (0, 1 - samp, me)

            def peer_of(dx, dy, dz):
                return nz[dz] * (SIDE * SIDE) + ny[dy] + nx[dx]

            def rows_of(index):
                return pl.ds(pl.multiple_of(index * chunk, chunk), chunk)

            w_copy = pltpu.make_async_copy(w_hbm, w_v, in_sem.at[0])
            w_copy.start()
            x_copies = []
            for order, dz in enumerate(FAR_FIRST):
                pair = []
                for side in range(2):
                    block = pl.ds(pl.multiple_of(side * half + nz[dz] * plane, plane), plane)
                    pair.append(pltpu.make_async_copy(x_hbm.at[block], x_v.at[block], x_sem.at[2 * order + side]))
                    pair[-1].start()
                x_copies.append(pair)
            y_copies = []
            for side in range(2):
                block = pl.ds(pl.multiple_of(side * half + me * chunk, chunk), chunk)
                y_copies.append(pltpu.make_async_copy(y_hbm.at[block], y_v.at[side], in_sem.at[1 + side]))
                y_copies[-1].start()

            barrier = pltpu.get_barrier_semaphore()
            pl.semaphore_signal(barrier, inc=1, device_id=sibling, device_id_type=MESH_ID)
            for dz in FAR_FIRST:
                for dx, dy in PLANE:
                    if (dx, dy, dz) != (0, 0, 0):
                        pl.semaphore_signal(barrier, inc=1, device_id=(0, samp, peer_of(dx, dy, dz)), device_id_type=MESH_ID)

            w_copy.wait()
            start = w_v[...]
            zero = jnp.zeros((feat_len, targets), bf16)
            wl[...] = jnp.concatenate([start.astype(bf16), zero], axis=1)
            wr[...] = jnp.concatenate([zero, start.astype(bf16)], axis=1)
            for col in range(feat_len // 128):
                wt[:, col * 128:(col + 1) * 128] = jnp.transpose(start[col * 128:(col + 1) * 128, :])
            for copy in y_copies:
                copy.wait()
            rown[...] = jnp.concatenate([y_v[0], y_v[1]], axis=1)

            def send_terms(before):
                for order, dz in enumerate(FAR_FIRST):
                    before(order)
                    left = pl.ds(pl.multiple_of(nz[dz] * plane, plane), plane)
                    right = pl.ds(pl.multiple_of(half + nz[dz] * plane, plane), plane)
                    term = jnp.dot(x_v[left, :], wl[...], preferred_element_type=f32)
                    term += jnp.dot(x_v[right, :], wr[...], preferred_element_type=f32)
                    ub[left, :] = term.astype(bf16)
                    for dx, dy in PLANE:
                        if (dx, dy, dz) == (0, 0, 0):
                            continue
                        peer = peer_of(dx, dy, dz)
                        pltpu.make_async_remote_copy(
                            src_ref=ub.at[rows_of(peer)], dst_ref=rs.at[rows_of(me)], send_sem=rs_send, recv_sem=rs_recv.at[dz],
                            device_id=(0, samp, peer), device_id_type=MESH_ID).start()
                rs[rows_of(me), :] = ub[rows_of(me), :]

            def wait_rows(ref, count, sem):
                block = ref.at[pl.ds(0, count)]
                pltpu.make_async_copy(block, block, sem).wait()

            def group(dz):
                return plane - chunk if dz == 0 else plane

            def reduce_terms(scale):
                for dz in NEAR_FIRST:
                    wait_rows(rs, group(dz), rs_recv.at[dz])
                total = rs[0:chunk, :].astype(f32)
                for index in range(1, feat_count):
                    total += rs[index * chunk:(index + 1) * chunk, :].astype(f32)
                rown[...] = rown[...] - scale * total

            def send_owned(src, dst):
                for dz in FAR_FIRST:
                    for dx, dy in PLANE:
                        if (dx, dy, dz) == (0, 0, 0):
                            continue
                        pltpu.make_async_remote_copy(
                            src_ref=src, dst_ref=dst.at[rows_of(me)], send_sem=ag_send, recv_sem=ag_recv.at[dz],
                            device_id=(0, samp, peer_of(dx, dy, dz)), device_id_type=MESH_ID).start()

            def from_plane(dz):
                return nz[(SIDE - dz) % SIDE]

            def sweep(step, unused):
                def before(order):
                    @pl.when(step == 0)
                    def _():
                        for copy in x_copies[order]:
                            copy.wait()
                        if order == 0:
                            pl.semaphore_wait(barrier, feat_count)

                send_terms(before)
                reduce_terms(jnp.where(step == 0, 1.0, COMBINE_WEIGHT))
                rb[rows_of(me), :] = rown[...].astype(bf16)
                send_owned(rb.at[rows_of(me)], rb)
                for place, dz in enumerate(NEAR_FIRST):
                    wait_rows(rb, group(dz), ag_recv.at[dz])
                    source = from_plane(dz)
                    left = pl.ds(pl.multiple_of(source * plane, plane), plane)
                    right = pl.ds(pl.multiple_of(half + source * plane, plane), plane)
                    turned = jnp.transpose(rb[left, :])
                    grad = jnp.dot(turned[:targets], x_v[left, :], preferred_element_type=f32)
                    grad += jnp.dot(turned[targets:], x_v[right, :], preferred_element_type=f32)
                    if place:
                        grad += gacc[...]
                    gacc[...] = grad
                slot = step % 2
                exchange = pltpu.make_async_remote_copy(
                    src_ref=gacc, dst_ref=gx.at[slot], send_sem=gx_send, recv_sem=gx_recv.at[slot],
                    device_id=sibling, device_id_type=MESH_ID)
                exchange.start()
                wait_rows(rs, half - chunk, rs_send)
                wait_rows(rs, half - chunk, ag_send)
                exchange.wait_recv()
                gradient = (gacc[...] + gx[slot]) * (1.0 / samples)
                delta = eta_ref[...] * (gradient - ridge * wt[...])
                wt[...] = wt[...] + COMBINE_WEIGHT * delta
                empty = jnp.zeros((targets, 128), f32)
                for col in range(feat_len // 128):
                    span = slice(col * 128, (col + 1) * 128)
                    wl[span, :] = jnp.transpose(jnp.concatenate([delta[:, span], empty], axis=0)).astype(bf16)
                    wr[span, :] = jnp.transpose(jnp.concatenate([empty, delta[:, span]], axis=0)).astype(bf16)
                exchange.wait_send()
                return 0

            lax.fori_loop(0, SWEEPS, sweep, 0)
            wt_copy = pltpu.make_async_copy(wt, wt_out, in_sem.at[0])
            wt_copy.start()
            send_terms(lambda order: None)
            reduce_terms(COMBINE_WEIGHT)
            rf[rows_of(me), :] = rown[...]
            send_owned(rf.at[rows_of(me)], rf)
            out_copies = []
            for dz in NEAR_FIRST:
                wait_rows(rf, group(dz), ag_recv.at[dz])
                block = pl.ds(pl.multiple_of(from_plane(dz) * plane, plane), plane)
                out_copies.append(pltpu.make_async_copy(rf.at[block], rp_out.at[block], out_sem.at[dz]))
                out_copies[-1].start()
            wait_rows(rs, half - chunk, rs_send)
            wait_rows(rf, half - chunk, ag_send)
            wt_copy.wait()
            for copy in out_copies:
                copy.wait()

        any_space = pl.BlockSpec(memory_space=pl.ANY)
        vmem = pl.BlockSpec(memory_space=pltpu.VMEM)
        return pl.pallas_call(
            kernel,
            name="ridge_sweeps",
            out_shape=(jax.ShapeDtypeStruct((targets, feat_len), f32), jax.ShapeDtypeStruct((half, lanes), f32)),
            in_specs=[any_space, any_space, any_space, vmem],
            out_specs=(any_space, any_space),
            scratch_shapes=[
                pltpu.VMEM((rows, feat_len), bf16),
                pltpu.VMEM((feat_len, targets), f32),
                pltpu.VMEM((2, chunk, targets), f32),
                pltpu.VMEM((half, lanes), bf16),
                pltpu.VMEM((half, lanes), bf16),
                pltpu.VMEM((half, lanes), bf16),
                pltpu.VMEM((chunk, lanes), f32),
                pltpu.VMEM((half, lanes), f32),
                pltpu.VMEM((targets, feat_len), f32),
                pltpu.VMEM((targets, feat_len), f32),
                pltpu.VMEM((2, targets, feat_len), f32),
                pltpu.VMEM((feat_len, lanes), bf16),
                pltpu.VMEM((feat_len, lanes), bf16),
                pltpu.SemaphoreType.DMA((2 * SIDE,)),
                pltpu.SemaphoreType.DMA((3,)),
                pltpu.SemaphoreType.DMA,
                pltpu.SemaphoreType.DMA((SIDE,)),
                pltpu.SemaphoreType.DMA,
                pltpu.SemaphoreType.DMA((SIDE,)),
                pltpu.SemaphoreType.DMA,
                pltpu.SemaphoreType.DMA((2,)),
                pltpu.SemaphoreType.DMA((SIDE,)),
            ],
            compiler_params=pltpu.CompilerParams(collective_id=0, has_side_effects=True),
        )

    def local_solve(x_loc, w_loc, y_loc, eta_loc):
        rows_loc, feat_len = x_loc.shape
        targets = w_loc.shape[1]
        samples = rows_loc * samp_count
        ridge = RIDGE_SCALE * (feat_len * feat_count) / samples
        call = make_kernel(rows_loc, feat_len, targets, ridge, samples)
        weights_turned, packed = call(x_loc, w_loc, y_loc, eta_loc.reshape(1, feat_len))
        residual = jnp.concatenate([packed[:, :targets], packed[:, targets:]], axis=0)
        return weights_turned.T, residual

    return jax.shard_map(
        local_solve,
        mesh=mesh,
        in_specs=(P(("prob", "samp"), "feat"), P(("prob", "feat"), None), P(("prob", "samp"), None), P(("prob", "feat"))),
        out_specs=(P(("prob", "feat"), None), P(("prob", "samp"), None)),
        check_vma=False,
    )
```

```python
import jax
import jax.numpy as jnp
from jax import lax
from jax.experimental import pallas as pl
from jax.experimental.pallas import tpu as pltpu
from jax.sharding import PartitionSpec as P

SWEEPS = 4
COMBINE_WEIGHT = 0.8
RIDGE_SCALE = 0.1
SIDE = 4
MESH_ID = pl.DeviceIdType.MESH

PLANE = sorted(
    [(dx, dy) for dy in range(SIDE) for dx in range(SIDE)],
    key=lambda d: -(min(d[0], SIDE - d[0]) + min(d[1], SIDE - d[1])),
)
FAR_FIRST = (2, 1, 3, 0)
NEAR_FIRST = (0, 1, 3, 2)
TURNED = (((1,), (1,)), ((), ()))


def solution(mesh):
    samp_count = mesh.shape["samp"]
    feat_count = mesh.shape["feat"]
    assert feat_count == SIDE**3 and samp_count == 2

    def make_kernel(rows, feat_len, targets, ridge, samples):
        plane = rows // SIDE
        tall = targets // SIDE
        wide = plane // SIDE
        f32, bf16 = jnp.float32, jnp.bfloat16

        def kernel(x_hbm, w_hbm, y_hbm, eta_ref, w_out, r_out, x_v, xt, ub, rs, rb, rown, wt, wb, gacc, gx,
                   x_sem, in_sem, rs_send, rs_recv, ag_send, ag_recv, gx_send, gx_recv):
            samp = lax.axis_index("samp")
            me = lax.axis_index("feat")
            cx, cy, cz = me % SIDE, (me // SIDE) % SIDE, me // (SIDE * SIDE)
            nx = [(cx + d) % SIDE for d in range(SIDE)]
            ny = [(cy + d) % SIDE for d in range(SIDE)]
            nz = [(cz + d) % SIDE for d in range(SIDE)]
            sibling = (0, 1 - samp, me)

            def peer_of(dx, dy, dz):
                return (0, samp, nz[dz] * (SIDE * SIDE) + ny[dy] * SIDE + nx[dx])

            def others(dz):
                return [(dx, dy) for dx, dy in PLANE if (dx, dy, dz) != (0, 0, 0)]

            def tall_at(x):
                return pl.ds(pl.multiple_of(x * tall, tall), tall)

            def wide_at(y):
                return pl.ds(pl.multiple_of(y * wide, wide), wide)

            def plane_at(z):
                return pl.ds(pl.multiple_of(z * plane, plane), plane)

            own_samples = pl.ds(pl.multiple_of(cz * plane + cy * wide, wide), wide)

            w_copy = pltpu.make_async_copy(w_hbm, wt, in_sem.at[0])
            w_copy.start()
            x_copies = []
            for order, dz in enumerate(FAR_FIRST):
                x_copies.append(pltpu.make_async_copy(x_hbm.at[plane_at(nz[dz])], x_v.at[plane_at(nz[dz])], x_sem.at[order]))
                x_copies[-1].start()
            y_copy = pltpu.make_async_copy(y_hbm.at[tall_at(cx), own_samples], rown, in_sem.at[1])
            y_copy.start()

            barrier = pltpu.get_barrier_semaphore()
            pl.semaphore_signal(barrier, inc=1, device_id=sibling, device_id_type=MESH_ID)
            for dz in FAR_FIRST:
                for dx, dy in others(dz):
                    pl.semaphore_signal(barrier, inc=1, device_id=peer_of(dx, dy, dz), device_id_type=MESH_ID)

            w_copy.wait()
            wb[...] = wt[...].astype(bf16)
            y_copy.wait()

            def send_terms(term_of):
                for order, dz in enumerate(FAR_FIRST):
                    term_of(order, nz[dz])
                    for dx, dy in others(dz):
                        pltpu.make_async_remote_copy(
                            src_ref=ub.at[nz[dz], tall_at(nx[dx]), wide_at(ny[dy])], dst_ref=rs.at[me], send_sem=rs_send,
                            recv_sem=rs_recv.at[dz], device_id=peer_of(dx, dy, dz), device_id_type=MESH_ID).start()
                rs[me] = ub[cz, tall_at(cx), wide_at(cy)]

            def later_term(order, z):
                ub[z] = jnp.dot(wb[...], xt[z], preferred_element_type=f32).astype(bf16)

            def wait_bytes(ref, sem):
                pltpu.make_async_copy(ref, ref, sem).wait()

            per_plane = SIDE * SIDE

            def group(dz):
                return per_plane - 1 if dz == 0 else per_plane

            def reduce_terms(scale):
                for dz in NEAR_FIRST:
                    wait_bytes(rs.at[pl.ds(0, group(dz))], rs_recv.at[dz])
                total = rs[0].astype(f32)
                for index in range(1, feat_count):
                    total += rs[index].astype(f32)
                rown[...] = rown[...] - scale * total

            def from_plane(dz):
                return nz[(SIDE - dz) % SIDE]

            def sweep(step, unused):
                def term_of(order, z):
                    @pl.when(step == 0)
                    def _():
                        x_copies[order].wait()
                        ub[z] = lax.dot_general(wb[...], x_v[plane_at(z), :], TURNED, preferred_element_type=f32).astype(bf16)
                        if order == 0:
                            pl.semaphore_wait(barrier, feat_count)

                    @pl.when(step > 0)
                    def _():
                        later_term(order, z)

                send_terms(term_of)

                @pl.when(step == 0)
                def _():
                    def turn(index, unused):
                        z, col = index // (feat_len // 128), index % (feat_len // 128)
                        lanes = pl.ds(pl.multiple_of(col * 128, 128), 128)
                        xt[z, lanes, :] = jnp.transpose(x_v[plane_at(z), lanes])
                        return 0

                    lax.fori_loop(0, SIDE * (feat_len // 128), turn, 0)

                reduce_terms(jnp.where(step == 0, 1.0, COMBINE_WEIGHT))
                mine = rb.at[cz, tall_at(cx), wide_at(cy)]
                mine[...] = rown[...].astype(bf16)
                for dz in FAR_FIRST:
                    for dx, dy in others(dz):
                        pltpu.make_async_remote_copy(
                            src_ref=mine, dst_ref=mine, send_sem=ag_send, recv_sem=ag_recv.at[dz],
                            device_id=peer_of(dx, dy, dz), device_id_type=MESH_ID).start()
                for place, dz in enumerate(NEAR_FIRST):
                    wait_bytes(rs.at[pl.ds(0, group(dz))], ag_recv.at[dz])
                    source = from_plane(dz)
                    grad = jnp.dot(rb[source], x_v[plane_at(source), :], preferred_element_type=f32)
                    if place:
                        grad += gacc[...]
                    gacc[...] = grad
                slot = step % 2
                exchange = pltpu.make_async_remote_copy(
                    src_ref=gacc, dst_ref=gx.at[slot], send_sem=gx_send, recv_sem=gx_recv.at[slot],
                    device_id=sibling, device_id_type=MESH_ID)
                exchange.start()
                wait_bytes(rs.at[pl.ds(0, feat_count - 1)], rs_send)
                wait_bytes(rs.at[pl.ds(0, feat_count - 1)], ag_send)
                exchange.wait_recv()
                gradient = (gacc[...] + gx[slot]) * (1.0 / samples)
                delta = eta_ref[...] * (gradient - ridge * wt[...])
                wt[...] = wt[...] + COMBINE_WEIGHT * delta
                wb[...] = delta.astype(bf16)
                exchange.wait_send()
                return 0

            lax.fori_loop(0, SWEEPS, sweep, 0)
            w_copy = pltpu.make_async_copy(wt, w_out, in_sem.at[0])
            w_copy.start()
            send_terms(later_term)
            reduce_terms(COMBINE_WEIGHT)
            mine = r_out.at[tall_at(cx), own_samples]
            y_copy = pltpu.make_async_copy(rown, mine, in_sem.at[1])
            y_copy.start()
            for dz in FAR_FIRST:
                for dx, dy in others(dz):
                    pltpu.make_async_remote_copy(
                        src_ref=rown, dst_ref=mine, send_sem=ag_send, recv_sem=ag_recv.at[dz],
                        device_id=peer_of(dx, dy, dz), device_id_type=MESH_ID).start()
            w_copy.wait()
            y_copy.wait()
            wait_bytes(rs.at[pl.ds(0, feat_count - 1)], rs_send)
            ratio = 2
            for dz in NEAR_FIRST:
                wait_bytes(rs.at[pl.ds(0, ratio * group(dz))], ag_recv.at[dz])
            sent = ratio * (feat_count - 1) * tall * wide // plane
            wait_bytes(xt.at[0, pl.ds(0, sent)], ag_send)

        any_space = pl.BlockSpec(memory_space=pl.ANY)
        vmem = pl.BlockSpec(memory_space=pltpu.VMEM)
        return pl.pallas_call(
            kernel,
            name="ridge_sweeps",
            out_shape=(jax.ShapeDtypeStruct((targets, feat_len), f32), jax.ShapeDtypeStruct((targets, rows), f32)),
            in_specs=[any_space, any_space, any_space, vmem],
            out_specs=(any_space, any_space),
            scratch_shapes=[
                pltpu.VMEM((rows, feat_len), bf16),
                pltpu.VMEM((SIDE, feat_len, plane), bf16),
                pltpu.VMEM((SIDE, targets, plane), bf16),
                pltpu.VMEM((feat_count, tall, wide), bf16),
                pltpu.VMEM((SIDE, targets, plane), bf16),
                pltpu.VMEM((tall, wide), f32),
                pltpu.VMEM((targets, feat_len), f32),
                pltpu.VMEM((targets, feat_len), bf16),
                pltpu.VMEM((targets, feat_len), f32),
                pltpu.VMEM((2, targets, feat_len), f32),
                pltpu.SemaphoreType.DMA((SIDE,)),
                pltpu.SemaphoreType.DMA((2,)),
                pltpu.SemaphoreType.DMA,
                pltpu.SemaphoreType.DMA((SIDE,)),
                pltpu.SemaphoreType.DMA,
                pltpu.SemaphoreType.DMA((SIDE,)),
                pltpu.SemaphoreType.DMA,
                pltpu.SemaphoreType.DMA((2,)),
            ],
            compiler_params=pltpu.CompilerParams(collective_id=0, has_side_effects=True),
        )

    def local_solve(x_loc, w_loc, y_loc, eta_loc):
        rows_loc, feat_len = x_loc.shape
        targets = w_loc.shape[1]
        samples = rows_loc * samp_count
        ridge = RIDGE_SCALE * (feat_len * feat_count) / samples
        call = make_kernel(rows_loc, feat_len, targets, ridge, samples)
        weights, residual = call(x_loc, w_loc.T, y_loc.T, eta_loc.reshape(1, feat_len))
        return weights.T, residual.T

    return jax.shard_map(
        local_solve,
        mesh=mesh,
        in_specs=(P(("prob", "samp"), "feat"), P(("prob", "feat"), None), P(("prob", "samp"), None), P(("prob", "feat"))),
        out_specs=(P(("prob", "feat"), None), P(("prob", "samp"), None)),
        check_vma=False,
    )
```

```python
import jax
import jax.numpy as jnp
from jax import lax
from jax.experimental import pallas as pl
from jax.experimental.pallas import tpu as pltpu
from jax.sharding import PartitionSpec as P

SWEEPS = 4
COMBINE_WEIGHT = 0.8
RIDGE_SCALE = 0.1
SIDE = 4
GROUPS = 2
MESH_ID = pl.DeviceIdType.MESH

PLANE = sorted(
    [(dx, dy) for dy in range(SIDE) for dx in range(SIDE)],
    key=lambda d: -(min(d[0], SIDE - d[0]) + min(d[1], SIDE - d[1])),
)
FAR_FIRST = (2, 1, 3, 0)
TURNED = (((1,), (1,)), ((), ()))


def solution(mesh):
    samp_count = mesh.shape["samp"]
    feat_count = mesh.shape["feat"]
    assert feat_count == SIDE**3 and samp_count == 2

    def make_kernel(rows, feat_len, targets, ridge, samples):
        f32, bf16 = jnp.float32, jnp.bfloat16
        plane = rows // SIDE
        height = targets // GROUPS
        tall = 16
        stacks = height // tall
        wide = plane * stacks // (SIDE * SIDE)
        per_plane = SIDE * SIDE

        def kernel(x_hbm, w_hbm, y_hbm, eta_ref, w_out, r_out, x_v, xt, ub, rs, rb, rown, wt, wb, gacc, gx,
                   x_sem, in_sem, y_sem, rs_send, rs_recv, ag_send, ag_recv, gx_send, gx_recv):
            samp = lax.axis_index("samp")
            me = lax.axis_index("feat")
            cx, cy, cz = me % SIDE, (me // SIDE) % SIDE, me // (SIDE * SIDE)
            nx = [(cx + d) % SIDE for d in range(SIDE)]
            ny = [(cy + d) % SIDE for d in range(SIDE)]
            nz = [(cz + d) % SIDE for d in range(SIDE)]
            sibling = (0, 1 - samp, me)
            tall_of = [pl.multiple_of((x % stacks) * tall, tall) for x in nx]
            wide_of = [x // stacks * wide for x in nx]
            lane_of = [y * (SIDE // stacks) * wide for y in ny]

            def peer_of(dx, dy, dz):
                return (0, samp, nz[dz] * per_plane + ny[dy] * SIDE + nx[dx])

            def others(dz):
                return [(dx, dy) for dx, dy in PLANE if (dx, dy, dz) != (0, 0, 0)]

            def chunk_of(dx, dy):
                return pl.ds(tall_of[dx], tall), pl.ds(pl.multiple_of(lane_of[dy] + wide_of[dx], wide), wide)

            def plane_at(z):
                return pl.ds(pl.multiple_of(z * plane, plane), plane)

            def output_at(group):
                lane = pl.multiple_of(cz * plane + lane_of[0] + wide_of[0], wide)
                return pl.ds(pl.multiple_of(group * height + tall_of[0], tall), tall), pl.ds(lane, wide)

            def group_rows(group):
                return slice(group * height, (group + 1) * height)

            def wait_bytes(ref, sem):
                pltpu.make_async_copy(ref, ref, sem).wait()

            def count(dz):
                return per_plane - 1 if dz == 0 else per_plane

            w_copy = pltpu.make_async_copy(w_hbm, wt, in_sem)
            w_copy.start()
            x_copies = []
            for order, dz in enumerate(FAR_FIRST):
                x_copies.append(pltpu.make_async_copy(x_hbm.at[plane_at(nz[dz])], x_v.at[plane_at(nz[dz])], x_sem.at[order]))
                x_copies[-1].start()
            y_copies = []
            for group in range(GROUPS):
                y_copies.append(pltpu.make_async_copy(y_hbm.at[output_at(group)], rown.at[group], y_sem.at[group]))
                y_copies[-1].start()

            barrier = pltpu.get_barrier_semaphore()
            pl.semaphore_signal(barrier, inc=1, device_id=sibling, device_id_type=MESH_ID)
            for dz in FAR_FIRST:
                for dx, dy in others(dz):
                    pl.semaphore_signal(barrier, inc=1, device_id=peer_of(dx, dy, dz), device_id_type=MESH_ID)

            def send_plane(group, dz):
                for dx, dy in others(dz):
                    pltpu.make_async_remote_copy(
                        src_ref=ub.at[(group, nz[dz], *chunk_of(dx, dy))], dst_ref=rs.at[group * feat_count + me], send_sem=rs_send.at[group],
                        recv_sem=rs_recv.at[group, dz], device_id=peer_of(dx, dy, dz), device_id_type=MESH_ID).start()

            def keep_own(group):
                rs[group * feat_count + me] = ub[(group, cz, *chunk_of(0, 0))]

            def send_terms(group):
                for dz in FAR_FIRST:
                    ub[group, nz[dz]] = jnp.dot(wb[group_rows(group), :], xt[nz[dz]], preferred_element_type=f32).astype(bf16)
                    send_plane(group, dz)
                keep_own(group)

            def reduce_terms(group, scale):
                for dz in FAR_FIRST:
                    wait_bytes(rs.at[pl.ds(0, count(dz))], rs_recv.at[group, dz])
                total = rs[group * feat_count].astype(f32)
                for index in range(1, feat_count):
                    total += rs[group * feat_count + index].astype(f32)
                rown[group] = rown[group] - scale * total

            def send_owned(group, src, dst):
                for dz in FAR_FIRST:
                    for dx, dy in others(dz):
                        pltpu.make_async_remote_copy(
                            src_ref=src, dst_ref=dst, send_sem=ag_send.at[group], recv_sem=ag_recv.at[group, dz],
                            device_id=peer_of(dx, dy, dz), device_id_type=MESH_ID).start()

            def share_residual(group):
                mine = rb.at[(group, cz, *chunk_of(0, 0))]
                mine[...] = rown[group].astype(bf16)
                send_owned(group, mine, mine)

            def step_weights(group, slot):
                for place, dz in enumerate(FAR_FIRST):
                    wait_bytes(rs.at[pl.ds(0, count(dz))], ag_recv.at[group, dz])
                    source = nz[(SIDE - dz) % SIDE]
                    grad = jnp.dot(rb[group, source], x_v[plane_at(source), :], preferred_element_type=f32)
                    if place:
                        grad += gacc[group]
                    gacc[group] = grad
                exchange = pltpu.make_async_remote_copy(
                    src_ref=gacc.at[group], dst_ref=gx.at[group, slot], send_sem=gx_send.at[group],
                    recv_sem=gx_recv.at[group, slot], device_id=sibling, device_id_type=MESH_ID)
                exchange.start()
                sent = rs.at[pl.ds(0, feat_count - 1)]
                wait_bytes(sent, rs_send.at[group])
                wait_bytes(sent, ag_send.at[group])
                exchange.wait_recv()
                part = group_rows(group)
                gradient = (gacc[group] + gx[group, slot]) * (1.0 / samples)
                delta = eta_ref[...] * (gradient - ridge * wt[part, :])
                wt[part, :] = wt[part, :] + COMBINE_WEIGHT * delta
                wb[part, :] = delta.astype(bf16)
                exchange.wait_send()

            w_copy.wait()
            wb[...] = wt[...].astype(bf16)
            for order, dz in enumerate(FAR_FIRST):
                x_copies[order].wait()
                first = lax.dot_general(wb[...], x_v[plane_at(nz[dz]), :], TURNED, preferred_element_type=f32)
                for group in range(GROUPS):
                    ub[group, nz[dz]] = first[group_rows(group), :].astype(bf16)
                if order == 0:
                    pl.semaphore_wait(barrier, feat_count)
                for group in range(GROUPS):
                    send_plane(group, dz)
            for group in range(GROUPS):
                keep_own(group)
                y_copies[group].wait()

            def turn(index, unused):
                z, col = index // (feat_len // 128), index % (feat_len // 128)
                lanes = pl.ds(pl.multiple_of(col * 128, 128), 128)
                xt[z, lanes, :] = jnp.transpose(x_v[plane_at(z), lanes])
                return 0

            lax.fori_loop(0, SIDE * (feat_len // 128), turn, 0)

            def sweep(step, unused):
                scale = jnp.where(step == 0, 1.0, COMBINE_WEIGHT)
                for group in range(GROUPS):
                    reduce_terms(group, scale)
                    share_residual(group)
                for group in range(GROUPS):
                    step_weights(group, step % 2)
                    send_terms(group)
                return 0

            lax.fori_loop(0, SWEEPS, sweep, 0)
            w_copy = pltpu.make_async_copy(wt, w_out, in_sem)
            w_copy.start()
            y_copies = []
            for group in range(GROUPS):
                reduce_terms(group, COMBINE_WEIGHT)
                mine = r_out.at[output_at(group)]
                y_copies.append(pltpu.make_async_copy(rown.at[group], mine, y_sem.at[group]))
                y_copies[-1].start()
                send_owned(group, rown.at[group], mine)
            w_copy.wait()
            ratio = 2
            for group in range(GROUPS):
                y_copies[group].wait()
                wait_bytes(rs.at[pl.ds(0, feat_count - 1)], rs_send.at[group])
                for dz in FAR_FIRST:
                    wait_bytes(rs.at[pl.ds(0, ratio * count(dz))], ag_recv.at[group, dz])
                wait_bytes(rs.at[pl.ds(0, ratio * (feat_count - 1))], ag_send.at[group])

        any_space = pl.BlockSpec(memory_space=pl.ANY)
        vmem = pl.BlockSpec(memory_space=pltpu.VMEM)
        return pl.pallas_call(
            kernel,
            name="ridge_sweeps",
            out_shape=(jax.ShapeDtypeStruct((targets, feat_len), f32), jax.ShapeDtypeStruct((targets, rows), f32)),
            in_specs=[any_space, any_space, any_space, vmem],
            out_specs=(any_space, any_space),
            scratch_shapes=[
                pltpu.VMEM((rows, feat_len), bf16),
                pltpu.VMEM((SIDE, feat_len, plane), bf16),
                pltpu.VMEM((GROUPS, SIDE, height, plane), bf16),
                pltpu.VMEM((GROUPS * feat_count, tall, wide), bf16),
                pltpu.VMEM((GROUPS, SIDE, height, plane), bf16),
                pltpu.VMEM((GROUPS, tall, wide), f32),
                pltpu.VMEM((targets, feat_len), f32),
                pltpu.VMEM((targets, feat_len), bf16),
                pltpu.VMEM((GROUPS, height, feat_len), f32),
                pltpu.VMEM((GROUPS, 2, height, feat_len), f32),
                pltpu.SemaphoreType.DMA((SIDE,)),
                pltpu.SemaphoreType.DMA,
                pltpu.SemaphoreType.DMA((GROUPS,)),
                pltpu.SemaphoreType.DMA((GROUPS,)),
                pltpu.SemaphoreType.DMA((GROUPS, SIDE)),
                pltpu.SemaphoreType.DMA((GROUPS,)),
                pltpu.SemaphoreType.DMA((GROUPS, SIDE)),
                pltpu.SemaphoreType.DMA((GROUPS,)),
                pltpu.SemaphoreType.DMA((GROUPS, 2)),
            ],
            compiler_params=pltpu.CompilerParams(collective_id=0, has_side_effects=True),
        )

    def local_solve(x_loc, w_loc, y_loc, eta_loc):
        rows_loc, feat_len = x_loc.shape
        targets = w_loc.shape[1]
        samples = rows_loc * samp_count
        ridge = RIDGE_SCALE * (feat_len * feat_count) / samples
        call = make_kernel(rows_loc, feat_len, targets, ridge, samples)
        weights, residual = call(x_loc, w_loc.T, y_loc.T, eta_loc.reshape(1, feat_len))
        return weights.T, residual.T

    return jax.shard_map(
        local_solve,
        mesh=mesh,
        in_specs=(P(("prob", "samp"), "feat"), P(("prob", "feat"), None), P(("prob", "samp"), None), P(("prob", "feat"))),
        out_specs=(P(("prob", "feat"), None), P(("prob", "samp"), None)),
        check_vma=False,
    )
```

```python
import jax
import jax.numpy as jnp
from jax import lax
from jax.experimental import pallas as pl
from jax.experimental.pallas import tpu as pltpu
from jax.sharding import PartitionSpec as P

SWEEPS = 4
COMBINE_WEIGHT = 0.8
RIDGE_SCALE = 0.1
SIDE = 4
GROUPS = 2
MESH_ID = pl.DeviceIdType.MESH

PLANE = sorted(
    [(dx, dy) for dy in range(SIDE) for dx in range(SIDE)],
    key=lambda d: -(min(d[0], SIDE - d[0]) + min(d[1], SIDE - d[1])),
)
FAR_FIRST = (2, 1, 3, 0)
TURNED = (((1,), (1,)), ((), ()))


def solution(mesh):
    samp_count = mesh.shape["samp"]
    feat_count = mesh.shape["feat"]
    assert feat_count == SIDE**3 and samp_count == 2

    def make_kernel(rows, feat_len, targets, ridge, samples):
        f32, bf16 = jnp.float32, jnp.bfloat16
        plane = rows // SIDE
        height = targets // GROUPS
        tall = 16
        stacks = height // tall
        wide = plane * stacks // (SIDE * SIDE)
        per_plane = SIDE * SIDE

        def kernel(x_hbm, w_hbm, y_hbm, eta_ref, w_out, r_out, x_v, xt, ub, rs, rb, rown, wt, wb, gacc, gx,
                   x_sem, in_sem, y_sem, rs_send, rs_recv, ag_send, ag_recv, gx_send, gx_recv):
            samp = lax.axis_index("samp")
            me = lax.axis_index("feat")
            cx, cy, cz = me % SIDE, (me // SIDE) % SIDE, me // (SIDE * SIDE)
            nx = [(cx + d) % SIDE for d in range(SIDE)]
            ny = [(cy + d) % SIDE for d in range(SIDE)]
            nz = [(cz + d) % SIDE for d in range(SIDE)]
            sibling = (0, 1 - samp, me)
            tall_of = [pl.multiple_of((x % stacks) * tall, tall) for x in nx]
            wide_of = [x // stacks * wide for x in nx]
            lane_of = [y * (SIDE // stacks) * wide for y in ny]

            def peer_of(dx, dy, dz):
                return (0, samp, nz[dz] * per_plane + ny[dy] * SIDE + nx[dx])

            def others(dz):
                return [(dx, dy) for dx, dy in PLANE if (dx, dy, dz) != (0, 0, 0)]

            def chunk_of(dx, dy):
                return pl.ds(tall_of[dx], tall), pl.ds(pl.multiple_of(lane_of[dy] + wide_of[dx], wide), wide)

            def plane_at(z):
                return pl.ds(pl.multiple_of(z * plane, plane), plane)

            def output_at(group):
                lane = pl.multiple_of(cz * plane + lane_of[0] + wide_of[0], wide)
                return pl.ds(pl.multiple_of(group * height + tall_of[0], tall), tall), pl.ds(lane, wide)

            def group_rows(group):
                return slice(group * height, (group + 1) * height)

            def wait_bytes(ref, sem):
                pltpu.make_async_copy(ref, ref, sem).wait()

            def count(dz):
                return per_plane - 1 if dz == 0 else per_plane

            w_copy = pltpu.make_async_copy(w_hbm, wt, in_sem)
            w_copy.start()
            x_copies = []
            for order, dz in enumerate(FAR_FIRST):
                x_copies.append(pltpu.make_async_copy(x_hbm.at[plane_at(nz[dz])], x_v.at[plane_at(nz[dz])], x_sem.at[order]))
                x_copies[-1].start()
            y_copies = []
            for group in range(GROUPS):
                y_copies.append(pltpu.make_async_copy(y_hbm.at[output_at(group)], rown.at[group], y_sem.at[group]))
                y_copies[-1].start()

            barrier = pltpu.get_barrier_semaphore()
            pl.semaphore_signal(barrier, inc=1, device_id=sibling, device_id_type=MESH_ID)
            for dz in FAR_FIRST:
                for dx, dy in others(dz):
                    pl.semaphore_signal(barrier, inc=1, device_id=peer_of(dx, dy, dz), device_id_type=MESH_ID)

            def send_plane(group, dz):
                for dx, dy in others(dz):
                    pltpu.make_async_remote_copy(
                        src_ref=ub.at[(group, nz[dz], *chunk_of(dx, dy))], dst_ref=rs.at[group * feat_count + me], send_sem=rs_send.at[group],
                        recv_sem=rs_recv.at[group, dz], device_id=peer_of(dx, dy, dz), device_id_type=MESH_ID).start()

            def keep_own(group):
                rs[group * feat_count + me] = ub[(group, cz, *chunk_of(0, 0))]

            def send_terms(group):
                for dz in FAR_FIRST:
                    ub[group, nz[dz]] = jnp.dot(wb[group_rows(group), :], xt[nz[dz]], preferred_element_type=f32).astype(bf16)
                    send_plane(group, dz)
                keep_own(group)

            def reduce_terms(group, scale):
                for dz in FAR_FIRST:
                    wait_bytes(rs.at[pl.ds(0, count(dz))], rs_recv.at[group, dz])
                total = rs[group * feat_count].astype(f32)
                for index in range(1, feat_count):
                    total += rs[group * feat_count + index].astype(f32)
                rown[group] = rown[group] - scale * total

            def send_owned(group, src, dst):
                for dz in FAR_FIRST:
                    for dx, dy in others(dz):
                        pltpu.make_async_remote_copy(
                            src_ref=src, dst_ref=dst, send_sem=ag_send.at[group], recv_sem=ag_recv.at[group, dz],
                            device_id=peer_of(dx, dy, dz), device_id_type=MESH_ID).start()

            def share_residual(group):
                mine = rb.at[(group, cz, *chunk_of(0, 0))]
                mine[...] = rown[group].astype(bf16)
                send_owned(group, mine, mine)

            def step_weights(group, slot):
                for place, dz in enumerate(FAR_FIRST):
                    wait_bytes(rs.at[pl.ds(0, count(dz))], ag_recv.at[group, dz])
                    source = nz[(SIDE - dz) % SIDE]
                    grad = jnp.dot(rb[group, source], x_v[plane_at(source), :], preferred_element_type=f32)
                    if place:
                        grad += gacc[group]
                    gacc[group] = grad
                exchange = pltpu.make_async_remote_copy(
                    src_ref=gacc.at[group], dst_ref=gx.at[group, slot], send_sem=gx_send.at[group],
                    recv_sem=gx_recv.at[group, slot], device_id=sibling, device_id_type=MESH_ID)
                exchange.start()
                sent = rs.at[pl.ds(0, feat_count - 1)]
                wait_bytes(sent, rs_send.at[group])
                wait_bytes(sent, ag_send.at[group])
                exchange.wait_recv()
                part = group_rows(group)
                gradient = (gacc[group] + gx[group, slot]) * (1.0 / samples)
                delta = eta_ref[...] * (gradient - ridge * wt[part, :])
                wt[part, :] = wt[part, :] + COMBINE_WEIGHT * delta
                wb[part, :] = delta.astype(bf16)
                exchange.wait_send()

            w_copy.wait()
            wb[...] = wt[...].astype(bf16)
            for order, dz in enumerate(FAR_FIRST):
                x_copies[order].wait()
                first = lax.dot_general(wb[...], x_v[plane_at(nz[dz]), :], TURNED, preferred_element_type=f32)
                for group in range(GROUPS):
                    ub[group, nz[dz]] = first[group_rows(group), :].astype(bf16)
                if order == 0:
                    pl.semaphore_wait(barrier, feat_count)
                send_plane(0, dz)
            for dz in FAR_FIRST:
                send_plane(1, dz)
            for group in range(GROUPS):
                keep_own(group)
                y_copies[group].wait()

            def turn(index, unused):
                z, col = index // (feat_len // 128), index % (feat_len // 128)
                lanes = pl.ds(pl.multiple_of(col * 128, 128), 128)
                xt[z, lanes, :] = jnp.transpose(x_v[plane_at(z), lanes])
                return 0

            lax.fori_loop(0, SIDE * (feat_len // 128), turn, 0)

            def sweep(step, unused):
                scale = jnp.where(step == 0, 1.0, COMBINE_WEIGHT)
                for group in range(GROUPS):
                    reduce_terms(group, scale)
                    share_residual(group)
                for group in range(GROUPS):
                    step_weights(group, step % 2)
                    send_terms(group)
                return 0

            lax.fori_loop(0, SWEEPS, sweep, 0)
            w_copy = pltpu.make_async_copy(wt, w_out, in_sem)
            w_copy.start()
            y_copies = []
            for group in range(GROUPS):
                reduce_terms(group, COMBINE_WEIGHT)
                mine = r_out.at[output_at(group)]
                y_copies.append(pltpu.make_async_copy(rown.at[group], mine, y_sem.at[group]))
                y_copies[-1].start()
                send_owned(group, rown.at[group], mine)
            w_copy.wait()
            ratio = 2
            for group in range(GROUPS):
                y_copies[group].wait()
                wait_bytes(rs.at[pl.ds(0, feat_count - 1)], rs_send.at[group])
                for dz in FAR_FIRST:
                    wait_bytes(rs.at[pl.ds(0, ratio * count(dz))], ag_recv.at[group, dz])
                wait_bytes(rs.at[pl.ds(0, ratio * (feat_count - 1))], ag_send.at[group])

        any_space = pl.BlockSpec(memory_space=pl.ANY)
        vmem = pl.BlockSpec(memory_space=pltpu.VMEM)
        return pl.pallas_call(
            kernel,
            name="ridge_sweeps",
            out_shape=(jax.ShapeDtypeStruct((targets, feat_len), f32), jax.ShapeDtypeStruct((targets, rows), f32)),
            in_specs=[any_space, any_space, any_space, vmem],
            out_specs=(any_space, any_space),
            scratch_shapes=[
                pltpu.VMEM((rows, feat_len), bf16),
                pltpu.VMEM((SIDE, feat_len, plane), bf16),
                pltpu.VMEM((GROUPS, SIDE, height, plane), bf16),
                pltpu.VMEM((GROUPS * feat_count, tall, wide), bf16),
                pltpu.VMEM((GROUPS, SIDE, height, plane), bf16),
                pltpu.VMEM((GROUPS, tall, wide), f32),
                pltpu.VMEM((targets, feat_len), f32),
                pltpu.VMEM((targets, feat_len), bf16),
                pltpu.VMEM((GROUPS, height, feat_len), f32),
                pltpu.VMEM((GROUPS, 2, height, feat_len), f32),
                pltpu.SemaphoreType.DMA((SIDE,)),
                pltpu.SemaphoreType.DMA,
                pltpu.SemaphoreType.DMA((GROUPS,)),
                pltpu.SemaphoreType.DMA((GROUPS,)),
                pltpu.SemaphoreType.DMA((GROUPS, SIDE)),
                pltpu.SemaphoreType.DMA((GROUPS,)),
                pltpu.SemaphoreType.DMA((GROUPS, SIDE)),
                pltpu.SemaphoreType.DMA((GROUPS,)),
                pltpu.SemaphoreType.DMA((GROUPS, 2)),
            ],
            compiler_params=pltpu.CompilerParams(collective_id=0, has_side_effects=True),
        )

    def local_solve(x_loc, w_loc, y_loc, eta_loc):
        rows_loc, feat_len = x_loc.shape
        targets = w_loc.shape[1]
        samples = rows_loc * samp_count
        ridge = RIDGE_SCALE * (feat_len * feat_count) / samples
        call = make_kernel(rows_loc, feat_len, targets, ridge, samples)
        weights, residual = call(x_loc, w_loc.T, y_loc.T, eta_loc.reshape(1, feat_len))
        return weights.T, residual.T

    return jax.shard_map(
        local_solve,
        mesh=mesh,
        in_specs=(P(("prob", "samp"), "feat"), P(("prob", "feat"), None), P(("prob", "samp"), None), P(("prob", "feat"))),
        out_specs=(P(("prob", "feat"), None), P(("prob", "samp"), None)),
        check_vma=False,
    )
```

```python
import jax
import jax.numpy as jnp
from jax import lax
from jax.experimental import pallas as pl
from jax.experimental.pallas import tpu as pltpu
from jax.sharding import PartitionSpec as P

SWEEPS = 4
COMBINE_WEIGHT = 0.8
RIDGE_SCALE = 0.1
SIDE = 4
GROUPS = 2
MESH_ID = pl.DeviceIdType.MESH

PLANE = sorted(
    [(dx, dy) for dy in range(SIDE) for dx in range(SIDE)],
    key=lambda d: -(min(d[0], SIDE - d[0]) + min(d[1], SIDE - d[1])),
)
FAR_FIRST = (2, 1, 3, 0)
TURNED = (((1,), (1,)), ((), ()))


def solution(mesh):
    samp_count = mesh.shape["samp"]
    feat_count = mesh.shape["feat"]
    assert feat_count == SIDE**3 and samp_count == 2

    def make_kernel(rows, feat_len, targets, ridge, samples):
        f32, bf16 = jnp.float32, jnp.bfloat16
        plane = rows // SIDE
        height = targets // GROUPS
        tall = 16
        stacks = height // tall
        wide = plane * stacks // (SIDE * SIDE)
        per_plane = SIDE * SIDE

        def kernel(x_hbm, w_hbm, y_hbm, eta_ref, out, x_v, xt, ub, rs, rb, rown, wt, wb, gacc, gx,
                   x_sem, in_sem, y_sem, rs_send, rs_recv, ag_send, ag_recv, gx_send, gx_recv):
            w_out = out.at[:, pl.ds(rows, feat_len)]
            r_out = out
            samp = lax.axis_index("samp")
            me = lax.axis_index("feat")
            cx, cy, cz = me % SIDE, (me // SIDE) % SIDE, me // (SIDE * SIDE)
            nx = [(cx + d) % SIDE for d in range(SIDE)]
            ny = [(cy + d) % SIDE for d in range(SIDE)]
            nz = [(cz + d) % SIDE for d in range(SIDE)]
            sibling = (0, 1 - samp, me)
            tall_of = [pl.multiple_of((x % stacks) * tall, tall) for x in nx]
            wide_of = [x // stacks * wide for x in nx]
            lane_of = [y * (SIDE // stacks) * wide for y in ny]

            def peer_of(dx, dy, dz):
                return (0, samp, nz[dz] * per_plane + ny[dy] * SIDE + nx[dx])

            def others(dz):
                return [(dx, dy) for dx, dy in PLANE if (dx, dy, dz) != (0, 0, 0)]

            def chunk_of(dx, dy):
                return pl.ds(tall_of[dx], tall), pl.ds(pl.multiple_of(lane_of[dy] + wide_of[dx], wide), wide)

            def plane_at(z):
                return pl.ds(pl.multiple_of(z * plane, plane), plane)

            def output_at(group):
                lane = pl.multiple_of(cz * plane + lane_of[0] + wide_of[0], wide)
                return pl.ds(pl.multiple_of(group * height + tall_of[0], tall), tall), pl.ds(lane, wide)

            def group_rows(group):
                return slice(group * height, (group + 1) * height)

            def wait_bytes(ref, sem):
                pltpu.make_async_copy(ref, ref, sem).wait()

            def count(dz):
                return per_plane - 1 if dz == 0 else per_plane

            w_copy = pltpu.make_async_copy(w_hbm, wt, in_sem)
            w_copy.start()
            x_copies = []
            for order, dz in enumerate(FAR_FIRST):
                x_copies.append(pltpu.make_async_copy(x_hbm.at[plane_at(nz[dz])], x_v.at[plane_at(nz[dz])], x_sem.at[order]))
                x_copies[-1].start()
            y_copies = []
            for group in range(GROUPS):
                y_copies.append(pltpu.make_async_copy(y_hbm.at[output_at(group)], rown.at[group], y_sem.at[group]))
                y_copies[-1].start()

            barrier = pltpu.get_barrier_semaphore()
            pl.semaphore_signal(barrier, inc=1, device_id=sibling, device_id_type=MESH_ID)
            for dz in FAR_FIRST:
                for dx, dy in others(dz):
                    pl.semaphore_signal(barrier, inc=1, device_id=peer_of(dx, dy, dz), device_id_type=MESH_ID)

            def send_plane(group, dz):
                for dx, dy in others(dz):
                    pltpu.make_async_remote_copy(
                        src_ref=ub.at[(group, nz[dz], *chunk_of(dx, dy))], dst_ref=rs.at[group * feat_count + me], send_sem=rs_send.at[group],
                        recv_sem=rs_recv.at[group, dz], device_id=peer_of(dx, dy, dz), device_id_type=MESH_ID).start()

            def keep_own(group):
                rs[group * feat_count + me] = ub[(group, cz, *chunk_of(0, 0))]

            def send_terms(group):
                for dz in FAR_FIRST:
                    ub[group, nz[dz]] = jnp.dot(wb[group_rows(group), :], xt[nz[dz]], preferred_element_type=f32).astype(bf16)
                    send_plane(group, dz)
                keep_own(group)

            def reduce_terms(group, scale):
                for dz in FAR_FIRST:
                    wait_bytes(rs.at[pl.ds(0, count(dz))], rs_recv.at[group, dz])
                total = rs[group * feat_count].astype(f32)
                for index in range(1, feat_count):
                    total += rs[group * feat_count + index].astype(f32)
                rown[group] = rown[group] - scale * total

            def send_owned(group, src, dst):
                for dz in FAR_FIRST:
                    for dx, dy in others(dz):
                        pltpu.make_async_remote_copy(
                            src_ref=src, dst_ref=dst, send_sem=ag_send.at[group], recv_sem=ag_recv.at[group, dz],
                            device_id=peer_of(dx, dy, dz), device_id_type=MESH_ID).start()

            def share_residual(group):
                mine = rb.at[(group, cz, *chunk_of(0, 0))]
                mine[...] = rown[group].astype(bf16)
                send_owned(group, mine, mine)

            def step_weights(group, slot):
                for place, dz in enumerate(FAR_FIRST):
                    wait_bytes(rs.at[pl.ds(0, count(dz))], ag_recv.at[group, dz])
                    source = nz[(SIDE - dz) % SIDE]
                    grad = jnp.dot(rb[group, source], x_v[plane_at(source), :], preferred_element_type=f32)
                    if place:
                        grad += gacc[group]
                    gacc[group] = grad
                exchange = pltpu.make_async_remote_copy(
                    src_ref=gacc.at[group], dst_ref=gx.at[group, slot], send_sem=gx_send.at[group],
                    recv_sem=gx_recv.at[group, slot], device_id=sibling, device_id_type=MESH_ID)
                exchange.start()
                exchange.wait_recv()
                part = group_rows(group)
                gradient = (gacc[group] + gx[group, slot]) * (1.0 / samples)
                delta = eta_ref[...] * (gradient - ridge * wt[part, :])
                wt[part, :] = wt[part, :] + COMBINE_WEIGHT * delta
                wb[part, :] = delta.astype(bf16)
                exchange.wait_send()
                sent = rs.at[pl.ds(0, feat_count - 1)]
                wait_bytes(sent, rs_send.at[group])
                wait_bytes(sent, ag_send.at[group])

            w_copy.wait()
            wb[...] = wt[...].astype(bf16)
            for order, dz in enumerate(FAR_FIRST):
                x_copies[order].wait()
                first = lax.dot_general(wb[...], x_v[plane_at(nz[dz]), :], TURNED, preferred_element_type=f32)
                for group in range(GROUPS):
                    ub[group, nz[dz]] = first[group_rows(group), :].astype(bf16)
                if order == 0:
                    pl.semaphore_wait(barrier, feat_count)
                send_plane(0, dz)
            for dz in FAR_FIRST:
                send_plane(1, dz)
            for group in range(GROUPS):
                keep_own(group)
                y_copies[group].wait()

            def turn(index, unused):
                z, col = index // (feat_len // 128), index % (feat_len // 128)
                lanes = pl.ds(pl.multiple_of(col * 128, 128), 128)
                xt[z, lanes, :] = jnp.transpose(x_v[plane_at(z), lanes])
                return 0

            lax.fori_loop(0, SIDE * (feat_len // 128), turn, 0)

            def sweep(step, unused):
                scale = jnp.where(step == 0, 1.0, COMBINE_WEIGHT)
                for group in range(GROUPS):
                    reduce_terms(group, scale)
                    share_residual(group)
                for group in range(GROUPS):
                    step_weights(group, step % 2)
                    send_terms(group)
                return 0

            lax.fori_loop(0, SWEEPS, sweep, 0)
            w_copy = pltpu.make_async_copy(wt, w_out, in_sem)
            w_copy.start()
            y_copies = []
            for group in range(GROUPS):
                reduce_terms(group, COMBINE_WEIGHT)
                mine = r_out.at[output_at(group)]
                y_copies.append(pltpu.make_async_copy(rown.at[group], mine, y_sem.at[group]))
                y_copies[-1].start()
                send_owned(group, rown.at[group], mine)
            w_copy.wait()
            ratio = 2
            for group in range(GROUPS):
                y_copies[group].wait()
                wait_bytes(rs.at[pl.ds(0, feat_count - 1)], rs_send.at[group])
                for dz in FAR_FIRST:
                    wait_bytes(rs.at[pl.ds(0, ratio * count(dz))], ag_recv.at[group, dz])
                wait_bytes(rs.at[pl.ds(0, ratio * (feat_count - 1))], ag_send.at[group])

        any_space = pl.BlockSpec(memory_space=pl.ANY)
        vmem = pl.BlockSpec(memory_space=pltpu.VMEM)
        return pl.pallas_call(
            kernel,
            name="ridge_sweeps",
            out_shape=jax.ShapeDtypeStruct((targets, rows + feat_len), f32),
            in_specs=[any_space, any_space, any_space, vmem],
            out_specs=any_space,
            scratch_shapes=[
                pltpu.VMEM((rows, feat_len), bf16),
                pltpu.VMEM((SIDE, feat_len, plane), bf16),
                pltpu.VMEM((GROUPS, SIDE, height, plane), bf16),
                pltpu.VMEM((GROUPS * feat_count, tall, wide), bf16),
                pltpu.VMEM((GROUPS, SIDE, height, plane), bf16),
                pltpu.VMEM((GROUPS, tall, wide), f32),
                pltpu.VMEM((targets, feat_len), f32),
                pltpu.VMEM((targets, feat_len), bf16),
                pltpu.VMEM((GROUPS, height, feat_len), f32),
                pltpu.VMEM((GROUPS, 2, height, feat_len), f32),
                pltpu.SemaphoreType.DMA((SIDE,)),
                pltpu.SemaphoreType.DMA,
                pltpu.SemaphoreType.DMA((GROUPS,)),
                pltpu.SemaphoreType.DMA((GROUPS,)),
                pltpu.SemaphoreType.DMA((GROUPS, SIDE)),
                pltpu.SemaphoreType.DMA((GROUPS,)),
                pltpu.SemaphoreType.DMA((GROUPS, SIDE)),
                pltpu.SemaphoreType.DMA((GROUPS,)),
                pltpu.SemaphoreType.DMA((GROUPS, 2)),
            ],
            compiler_params=pltpu.CompilerParams(collective_id=0, has_side_effects=True),
        )

    def local_solve(x_loc, w_loc, y_loc, eta_loc):
        rows_loc, feat_len = x_loc.shape
        targets = w_loc.shape[1]
        samples = rows_loc * samp_count
        ridge = RIDGE_SCALE * (feat_len * feat_count) / samples
        call = make_kernel(rows_loc, feat_len, targets, ridge, samples)
        both = call(x_loc, w_loc.T, y_loc.T, eta_loc.reshape(1, feat_len))
        return both[:, rows_loc:].T, both[:, :rows_loc].T

    return jax.shard_map(
        local_solve,
        mesh=mesh,
        in_specs=(P(("prob", "samp"), "feat"), P(("prob", "feat"), None), P(("prob", "samp"), None), P(("prob", "feat"))),
        out_specs=(P(("prob", "feat"), None), P(("prob", "samp"), None)),
        check_vma=False,
    )
```
